32 devices in a mesh: prow: 4 (over z), pcol: 8 (over y, x, core).
Axes of the slice: x: 2, y: 2, z: 4, core: 2. Of those that a mesh axis runs over, the one named last changes fastest.
Arguments:
- points: float32 [1, 8, 2, 1024], P(None, 'pcol'), may hold values from 0 to 1
- range_length: float32 [1], replicated, may hold values from 0.05 to 0.15
- smoothness: int32 [1], replicated, may hold values from 0 to 2
- sketch_bank: bfloat16 [8, 48, 1024], P('pcol'), may hold values from -6 to 6
- sketch_ids: int32 [2, 4, 1, 8], P(None, 'prow', None, 'pcol'), may hold values from 0 to 7
- tile_ranks: int32 [2, 4, 1, 8], P(None, 'prow', None, 'pcol'), may hold values from 16 to 48
Outputs:
- y_factors: float32 [2, 4, 1, 8, 48, 1024], P(None, 'prow', None, 'pcol')
- c_factors: float32 [2, 4, 1, 8, 48, 1024], P(None, 'prow', None, 'pcol')
- tile_error: float32 [2, 4, 1, 8], P(None, 'prow', None, 'pcol')
- rank_total: int32 [1], replicated
The draws below stay inside these ranges and needn't reach their ends.
All inputs are finite; a program needn't handle non-finite values.
Results may differ from the reference program's by a relative error of at most 0.0098.
The reference program's roundings to bfloat16 on the way count: a program that leaves them out, or rounds other values in their place, can miss the bound.
Values may be sent and summed in bfloat16 or wider, within the bound.
A program may use at most 64 MiB of HBM per device.

```python
import math
import jax
import jax.numpy as jnp
import numpy as np
from jax import lax

NB = 1024
RMAX = 48
RMIN = 16
MTB = 1
MT = 8
TRD = 2
SB = 8
N_PROW = 4
N_PCOL = 8


def draw_points(key, part):
    total_bits = max(1, (MT - 1).bit_length())
    x_bits = (total_bits + 1) // 2
    y_bits = total_bits // 2
    blocks = jnp.arange(MT, dtype=jnp.int32)
    cell_x = jnp.zeros((MT,), jnp.float32)
    cell_y = jnp.zeros((MT,), jnp.float32)
    for level in range(total_bits):
        digit = (blocks // 2 ** level % 2).astype(jnp.float32)
        if level % 2 == 0:
            cell_x = cell_x + digit * float(2 ** (level // 2))
        else:
            cell_y = digit
    key_jitter = jax.random.fold_in(key, 11)
    key_spread = jax.random.fold_in(key, 23)
    key_select = jax.random.fold_in(key, 37)
    jitter = jax.random.uniform(key_jitter, (MT, 2, NB), jnp.float32)
    spread = jax.random.uniform(key_spread, (MT, 2, NB), jnp.float32)
    select = jax.random.uniform(key_select, (MT, 1, NB), jnp.float32)
    share = 0.25
    coord_x = (cell_x[:, None] + jitter[:, 0]) / float(2 ** x_bits)
    coord_y = (cell_y[:, None] + jitter[:, 1]) / float(2 ** y_bits)
    local = jnp.stack([coord_x, coord_y], axis=1)
    placed = jnp.where(select < share, spread, local)
    return placed.reshape(MTB, N_PCOL, 2, NB)


def plant(drawn, key, low, largest):
    longest = drawn.shape.index(max(drawn.shape))
    spots = []
    for shift in (0, 1):
        where = [jax.random.randint(jax.random.fold_in(key, axis), (), 0, length) for axis, length in enumerate(drawn.shape)]
        where[longest] = (where[longest] + shift) % drawn.shape[longest]
        spots.append(tuple(where))
    return drawn.at[spots[0]].set(low).at[spots[1]].set(largest)


def block_levels(stream_key, extent, shards, least, high):
    def one(axis_at, parts):
        heights = jax.random.uniform(jax.random.fold_in(jax.random.fold_in(stream_key, 6), axis_at), (parts,), jnp.float32, least / len(shards), high / len(shards))
        return jnp.repeat(jnp.exp(heights), extent[axis_at] // parts).reshape((-1,) + (1,) * (len(extent) - axis_at - 1))

    gain = one(*shards[0])
    for cut in shards[1:]:
        gain = gain * one(*cut)
    return gain


def noise(rng, shape, scale, reach, cuts=(), held_as=jnp.bfloat16):
    entries = scale * jax.random.normal(rng, shape, jnp.float32)
    if cuts:
        entries = entries * block_levels(rng, shape, cuts, -0.22, 0.18)
    return jnp.clip(entries, -reach, reach).astype(held_as)


def setup_inputs(seed: int = 0) -> dict:
    key_list = jax.random.split(jax.random.key(seed), 7)
    points = draw_points(jax.random.fold_in(key_list[6], 71), 0)
    range_length = jnp.clip(jnp.exp(jax.random.uniform(key_list[1], (1,), jnp.float32, math.log(0.05), math.log(0.15))), 0.05, 0.15)
    smoothness = jax.random.randint(key_list[2], (1,), 0, 3).astype(jnp.int32)
    sketch_bank = noise(key_list[3], (SB, RMAX, NB), 1.0, 6.0, ((0, 8),))
    sketch_ids = plant(jax.random.randint(key_list[4], (TRD, N_PROW, MTB, N_PCOL), 0, SB), jax.random.fold_in(key_list[4], 1), 0, SB - 1).astype(jnp.int32)
    tile_ranks = plant(jax.random.randint(key_list[5], (TRD, N_PROW, MTB, N_PCOL), RMIN, RMAX + 1), jax.random.fold_in(key_list[5], 1), RMIN, RMAX).astype(jnp.int32)
    return dict(points=points, range_length=range_length, smoothness=smoothness, sketch_bank=sketch_bank, sketch_ids=sketch_ids, tile_ranks=tile_ranks)


def kernel_factors(smoothness, range_length):
    morton_value = smoothness[0].astype(jnp.float32)
    kernel_scale = jnp.sqrt(2.0 * morton_value + 1.0) / range_length[0]
    linear_factor = jnp.where(smoothness[0] >= 1, 1.0, 0.0).astype(jnp.float32)
    squared_distance = jnp.where(smoothness[0] >= 2, 1.0 / 3.0, 0.0).astype(jnp.float32)
    return (kernel_scale, linear_factor, squared_distance)

def covariance_tile(row_locations, column_locations, kernel_scale, linear_factor, squared_distance):
    offset_horizontal = row_locations[0][:, None] - column_locations[0][None, :]
    offset_vertical = row_locations[1][:, None] - column_locations[1][None, :]
    scaled_distance = kernel_scale * jnp.sqrt(offset_horizontal * offset_horizontal + offset_vertical * offset_vertical)
    return (1.0 + linear_factor * scaled_distance + squared_distance * scaled_distance * scaled_distance) * jnp.exp(-scaled_distance)

def compress(tile_low, sketch, rank):
    keep = jnp.arange(sketch.shape[0]) < rank
    sketch = jnp.where(keep[:, None], sketch, jnp.zeros_like(sketch))
    sketched = lax.dot_general(sketch.astype(jnp.float32), tile_low.astype(jnp.float32), (((1,), (1,)), ((), ())), preferred_element_type=jnp.float32)
    product = jnp.dot(sketched.astype(jnp.bfloat16).astype(jnp.float32), tile_low.astype(jnp.float32), preferred_element_type=jnp.float32)
    gram = jnp.dot(sketched, sketched.T, precision=lax.Precision.HIGHEST)
    shift = 0.1 * jnp.trace(gram) / rank.astype(jnp.float32)
    gram = gram + jnp.diag(jnp.where(keep, shift, jnp.ones_like(shift)))
    factor = jnp.linalg.cholesky(gram)
    coeffs = jax.scipy.linalg.cho_solve((factor, True), product)
    approx = lax.dot_general(sketched, coeffs, (((0,), (0,)), ((), ())), precision=lax.Precision.HIGHEST)
    error = tile_low.astype(jnp.float32) - approx
    return (sketched, coeffs, jnp.sum(error * error))

def reference(points, range_length, smoothness, sketch_bank, sketch_ids, tile_ranks):
    every_block = points.reshape(MT, 2, NB)
    kernel_scale, linear_factor, squared_distance = kernel_factors(smoothness, range_length)
    pairs = np.array([(row, col) for row in range(MT) for col in range(row + 1)], np.int32)
    row_index = jnp.asarray(pairs[:, 0]).astype(jnp.int32)
    col_index = jnp.asarray(pairs[:, 1]).astype(jnp.int32)
    row_major = row_index // N_PROW
    row_minor = row_index % N_PROW
    col_major = col_index // N_PCOL
    col_minor = col_index % N_PCOL
    chosen_ids = sketch_ids[row_major, row_minor, col_major, col_minor]
    chosen_ranks = tile_ranks[row_major, row_minor, col_major, col_minor]

    def one_tile(inputs):
        row_number, column_number, sketch_id, rank = inputs
        tile_block = covariance_tile(every_block[row_number], every_block[column_number], kernel_scale, linear_factor, squared_distance)
        norm_sq = jnp.sum(tile_block * tile_block)
        tile_low = tile_block.astype(jnp.bfloat16)
        sketched, coeffs, err_sq = compress(tile_low, sketch_bank[sketch_id], rank)
        return (sketched, coeffs, norm_sq, err_sq)
    sketched_all, coeffs_all, norm_all, err_all = lax.map(one_tile, (row_index, col_index, chosen_ids, chosen_ranks))
    offdiag = row_index > col_index
    total = jnp.sum(jnp.where(offdiag, 2.0, 1.0) * norm_all)
    errors = jnp.where(offdiag, jnp.sqrt(err_all), jnp.sqrt(norm_all)) * MT / jnp.sqrt(total)
    shape_out = (TRD, N_PROW, MTB, N_PCOL, RMAX, NB)
    y_out = jnp.zeros(shape_out, jnp.float32).at[row_major, row_minor, col_major, col_minor].set(jnp.where(offdiag[:, None, None], sketched_all, 0.0))
    c_out = jnp.zeros(shape_out, jnp.float32).at[row_major, row_minor, col_major, col_minor].set(jnp.where(offdiag[:, None, None], coeffs_all, 0.0))
    err_out = jnp.zeros((TRD, N_PROW, MTB, N_PCOL), jnp.float32).at[row_major, row_minor, col_major, col_minor].set(errors)
    rank_out = jnp.sum(jnp.where(offdiag, chosen_ranks, 0)).astype(jnp.int32).reshape(1)
    return (y_out, c_out, err_out, rank_out)
```

```python
import functools
import math

import jax
import jax.numpy as jnp
from jax import lax
from jax.experimental import pallas as pl
from jax.experimental.pallas import tpu as pltpu
from jax.sharding import PartitionSpec as P

MESH = pl.DeviceIdType.MESH
LOG2E = math.log2(math.e)
F32 = jnp.float32
BF16 = jnp.bfloat16
HIGH = lax.Precision.HIGHEST


def dot(a, b, da, db, precision=None):
    return lax.dot_general(
        a, b, (((da,), (db,)), ((), ())), preferred_element_type=F32, precision=precision
    )


def split(x):
    high = x.astype(BF16)
    return high, (x - high.astype(F32)).astype(BF16)


def all_sum(x):
    return jnp.sum(jnp.sum(x, axis=1, keepdims=True), axis=0, keepdims=True)


def invert(mats):
    size = mats[0].shape[0]
    row_at = lax.broadcasted_iota(jnp.int32, (size, size), 0)
    col_at = lax.broadcasted_iota(jnp.int32, (size, size), 1)
    for k in range(size):
        following = []
        for m in mats:
            col = jnp.broadcast_to(m[:, k : k + 1], (size, size))
            inverse = 1.0 / col[k : k + 1, :]
            row = jnp.where(col_at[:1] == k, 1.0, m[k : k + 1, :]) * inverse
            rest = jnp.where(col_at == k, 0.0, m) - col * row
            following.append(jnp.where(row_at == k, row, rest))
        mats = following
    return mats


def kernel(
    rows,
    cols,
    row_tiles,
    col_tiles,
    points,
    range_length,
    smoothness,
    bank,
    ids,
    ranks,
    y_out,
    c_out,
    err_out,
    rank_out,
    all_points,
    all_bank,
    low,
    norms,
    residuals,
    mine,
    col_sums,
    partial,
    row_sums,
    sem_local,
    sem_ps,
    sem_pr,
    sem_bs,
    sem_br,
    sem_cs,
    sem_cr,
    sem_rs,
    sem_rr,
):
    p = lax.axis_index("prow")
    q = lax.axis_index("pcol")
    per_bank, sketch_rows, size = bank.shape
    across = cols * col_tiles
    slots = [(a, b) for a in range(row_tiles) for b in range(col_tiles)]
    sibling = q + 1 - 2 * lax.rem(q, 2)

    barrier = pltpu.get_barrier_semaphore()
    for step in range(1, cols):
        pl.semaphore_signal(
            barrier, device_id=(p, lax.rem(q + step, cols)), device_id_type=MESH
        )
    for step in range(1, rows):
        pl.semaphore_signal(
            barrier, device_id=(lax.rem(p + step, rows), q), device_id_type=MESH
        )
    own_points = pltpu.make_async_copy(points.at[:, 0], all_points.at[q], sem_local.at[0])
    own_bank = pltpu.make_async_copy(
        bank, all_bank.at[pl.ds(q * per_bank, per_bank)], sem_local.at[1]
    )
    own_points.start()
    own_bank.start()
    pl.semaphore_wait(barrier, cols + rows - 2)

    def point_copy(source, target):
        return pltpu.make_async_remote_copy(
            src_ref=points.at[:, 0],
            dst_ref=all_points.at[source],
            send_sem=sem_ps.at[target],
            recv_sem=sem_pr.at[source],
            device_id=(p, target),
            device_id_type=MESH,
        )

    def bank_copy(block, target, send):
        return pltpu.make_async_remote_copy(
            src_ref=all_bank.at[pl.ds(block * per_bank, per_bank)] if send >= cols else bank,
            dst_ref=all_bank.at[pl.ds(block * per_bank, per_bank)],
            send_sem=sem_bs.at[send],
            recv_sem=sem_br.at[block],
            device_id=(p, target),
            device_id_type=MESH,
        )

    for step in range(1, cols):
        point_copy(q, lax.rem(q + step, cols)).start()
    for step in range(2, cols, 2):
        bank_copy(q, lax.rem(q + step, cols), step).start()
    bank_copy(q, sibling, 1).start()

    degree = jnp.full((8, 128), smoothness[0].astype(F32))
    scale = (LOG2E * jnp.sqrt(2.0 * degree + 1.0)) / jnp.full((8, 128), range_length[0])
    scale = scale[:1]
    linear = jnp.where(smoothness[0] >= 1, 1.0 / LOG2E, 0.0).astype(F32)
    square = jnp.where(smoothness[0] >= 2, 1.0 / (3.0 * LOG2E * LOG2E), 0.0).astype(F32)

    own_points.wait()
    for step in range(1, cols):
        point_copy(lax.rem(q + step, cols), q).wait_recv()

    def place(slot):
        a, b = slots[slot]
        return a * rows + p, b * cols + q

    def generate(slot):
        i, j = place(slot)

        @pl.when(j > i)
        def _():
            norms[slot] = jnp.zeros((8, 128), F32)

        @pl.when(j <= i)
        def _():
            row_block = lax.rem(i, cols)
            row_major = i // cols
            col_major = slots[slot][1]

            def chunk(c, total):
                at = pl.ds(pl.multiple_of(c * 128, 128), 128)
                x_row = all_points[row_block, row_major, 0:1, at] * scale
                y_row = all_points[row_block, row_major, 1:2, at] * scale
                x_row = jnp.broadcast_to(x_row, (128, 128)).T
                y_row = jnp.broadcast_to(y_row, (128, 128)).T
                for n in range(size // 128):
                    cut = slice(n * 128, n * 128 + 128)
                    x_col = points[col_major, 0, 0:1, cut] * scale
                    y_col = points[col_major, 0, 1:2, cut] * scale
                    dx = x_row - x_col
                    dy = y_row - y_col
                    d2 = dx * dx + dy * dy
                    t = d2 * lax.rsqrt(jnp.maximum(d2, 1e-30))
                    tile = (1.0 + linear * t + square * d2) * jnp.exp2(-t)
                    low[slot, at, cut] = tile.astype(BF16)
                    total = total + jnp.sum((tile * tile).reshape(16, 8, 128), axis=0)
                return total

            norms[slot] = lax.fori_loop(0, size // 128, chunk, jnp.zeros((8, 128), F32))

    generate(0)
    for step in range(2, cols, 2):
        block = lax.rem(q + step, cols)
        bank_copy(block, q, 0).wait_recv()
        bank_copy(block, sibling, cols + step).start()
    for slot in range(1, len(slots)):
        generate(slot)

    norm_sum = jnp.zeros((1, 1), F32)
    rank_sum = jnp.float32(0)
    for slot, (a, b) in enumerate(slots):
        i, j = place(slot)
        weight = jnp.where(j < i, 2.0, 1.0).astype(F32)
        norm_sum = norm_sum + weight * all_sum(norms[slot])
        rank_sum = rank_sum + jnp.where(j < i, ranks[a, 0, b, 0], 0).astype(F32)
    first = lax.broadcasted_iota(jnp.int32, (8, 128), 0) == 0
    mine[...] = jnp.where(first, jnp.broadcast_to(norm_sum, (8, 128)), rank_sum)

    own_bank.wait()
    bank_copy(sibling, q, 0).wait_recv()
    for step in range(2, cols, 2):
        bank_copy(lax.rem(sibling + step, cols), q, 0).wait_recv()

    def keep_of(a, b):
        return lax.broadcasted_iota(jnp.int32, (sketch_rows, 1), 0) < ranks[a, 0, b, 0]

    for slot, (a, b) in enumerate(slots):
        i, j = place(slot)

        @pl.when(j < i)
        def _():
            sketch = all_bank[ids[a, 0, b, 0]]
            sketch = jnp.where(keep_of(a, b), sketch.astype(F32), 0.0).astype(BF16)
            y_out[a, 0, b, 0] = dot(sketch, low[slot], 1, 1)

        @pl.when(j >= i)
        def _():
            y_out[a, 0, b, 0] = jnp.zeros((sketch_rows, size), F32)
            c_out[a, 0, b, 0] = jnp.zeros((sketch_rows, size), F32)
            residuals[slot] = norms[slot]

    def row_copy(source, target):
        return pltpu.make_async_remote_copy(
            src_ref=mine,
            dst_ref=row_sums.at[source],
            send_sem=sem_rs.at[target],
            recv_sem=sem_rr.at[source],
            device_id=(target, q),
            device_id_type=MESH,
        )

    def col_copy(source, target):
        return pltpu.make_async_remote_copy(
            src_ref=partial,
            dst_ref=col_sums.at[source],
            send_sem=sem_cs.at[target],
            recv_sem=sem_cr.at[source],
            device_id=(p, target),
            device_id_type=MESH,
        )

    for step in range(1, rows):
        row_copy(p, lax.rem(p + step, rows)).start()

    eye = lax.broadcasted_iota(jnp.int32, (sketch_rows, sketch_rows), 0) == (
        lax.broadcasted_iota(jnp.int32, (sketch_rows, sketch_rows), 1)
    )
    grams = []
    for slot, (a, b) in enumerate(slots):
        i, j = place(slot)
        y = y_out[a, 0, b, 0]
        gram = dot(y, y, 1, 1, HIGH)
        rank = jnp.full((1, 1), ranks[a, 0, b, 0].astype(F32))
        shift = 0.1 * all_sum(jnp.where(eye, gram, 0.0)) / rank
        diagonal = jnp.where(keep_of(a, b) & (j < i), shift, 1.0)
        grams.append(gram + jnp.where(eye, diagonal, 0.0))
    inverses = invert(grams)

    summed = mine[...]
    for step in range(1, rows):
        source = lax.rem(p + step, rows)
        row_copy(source, p).wait_recv()
        summed = summed + row_sums[source]
    partial[...] = summed

    for slot, (a, b) in enumerate(slots):
        i, j = place(slot)

        @pl.when(j < i)
        def _():
            product = dot(y_out[a, 0, b, 0].astype(BF16), low[slot], 1, 0)
            c_out[a, 0, b, 0] = dot(inverses[slot], product, 1, 0, HIGH)

    for step in range(1, cols):
        col_copy(q, lax.rem(q + step, cols)).start()

    for slot, (a, b) in enumerate(slots):
        i, j = place(slot)

        @pl.when(j < i)
        def _():
            y_high, y_low = split(y_out[a, 0, b, 0])
            c_high, c_low = split(c_out[a, 0, b, 0])
            left = jnp.concatenate([y_high, y_high, y_low], axis=0)
            right = jnp.concatenate([c_high, c_low, c_high], axis=0)
            total = jnp.zeros((8, 128), F32)
            for m in range(size // 128):
                cut = slice(m * 128, m * 128 + 128)
                gap = low[slot, cut].astype(F32) - dot(left[:, cut], right, 0, 0)
                gap = gap * gap
                for n in range(size // 128):
                    total = total + jnp.sum(
                        gap[:, n * 128 : n * 128 + 128].reshape(16, 8, 128), axis=0
                    )
            residuals[slot] = total

    whole = partial[...]
    for step in range(1, cols):
        source = lax.rem(q + step, cols)
        col_copy(source, q).wait_recv()
        whole = whole + col_sums[source]
    total = whole[0:1, 0:1]
    for slot, (a, b) in enumerate(slots):
        i, j = place(slot)
        error = jnp.sqrt(all_sum(residuals[slot])) * float(across) / jnp.sqrt(total)
        err_out[a, 0, b, 0] = jnp.where(j <= i, error, 0.0)[0, 0]
    rank_out[0] = whole[1:2, 0:1].astype(jnp.int32)[0, 0]

    for step in range(1, cols):
        target = lax.rem(q + step, cols)
        point_copy(q, target).wait_send()
        col_copy(q, target).wait_send()
    for step in range(2, cols, 2):
        bank_copy(q, lax.rem(q + step, cols), step).wait_send()
        bank_copy(lax.rem(q + step, cols), sibling, cols + step).wait_send()
    bank_copy(q, sibling, 1).wait_send()
    for step in range(1, rows):
        row_copy(p, lax.rem(p + step, rows)).wait_send()


def per_device(rows, cols, points, range_length, smoothness, bank, ids, ranks):
    row_tiles, col_tiles = ids.shape[0], ids.shape[2]
    per_bank, sketch_rows, size = bank.shape
    slots = row_tiles * col_tiles
    factors = jax.ShapeDtypeStruct((row_tiles, 1, col_tiles, 1, sketch_rows, size), F32)
    vmem = pl.BlockSpec(memory_space=pltpu.VMEM)
    smem = pl.BlockSpec(memory_space=pltpu.SMEM)
    dma = pltpu.SemaphoreType.DMA
    return pl.pallas_call(
        functools.partial(kernel, rows, cols, row_tiles, col_tiles),
        out_shape=(
            factors,
            factors,
            jax.ShapeDtypeStruct((row_tiles, 1, col_tiles, 1), F32),
            jax.ShapeDtypeStruct((1,), jnp.int32),
        ),
        in_specs=[vmem, smem, smem, vmem, smem, smem],
        out_specs=(vmem, vmem, smem, smem),
        scratch_shapes=[
            pltpu.VMEM((cols, col_tiles, 2, size), F32),
            pltpu.VMEM((cols * per_bank, sketch_rows, size), BF16),
            pltpu.VMEM((slots, size, size), BF16),
            pltpu.VMEM((slots, 8, 128), F32),
            pltpu.VMEM((slots, 8, 128), F32),
            pltpu.VMEM((8, 128), F32),
            pltpu.VMEM((cols, 8, 128), F32),
            pltpu.VMEM((8, 128), F32),
            pltpu.VMEM((rows, 8, 128), F32),
            dma((2,)),
            dma((cols,)),
            dma((cols,)),
            dma((2 * cols,)),
            dma((cols,)),
            dma((cols,)),
            dma((cols,)),
            dma((rows,)),
            dma((rows,)),
        ],
        compiler_params=pltpu.CompilerParams(
            collective_id=0, has_side_effects=True, vmem_limit_bytes=48 * 1024 * 1024
        ),
        name="tiles",
    )(points, range_length, smoothness, bank, ids, ranks)


def solution(mesh):
    in_specs = (
        P(None, "pcol", None, None),
        P(),
        P(),
        P("pcol", None, None),
        P(None, "prow", None, "pcol"),
        P(None, "prow", None, "pcol"),
    )
    out_specs = (
        P(None, "prow", None, "pcol", None, None),
        P(None, "prow", None, "pcol", None, None),
        P(None, "prow", None, "pcol"),
        P(),
    )
    return jax.shard_map(
        functools.partial(per_device, mesh.shape["prow"], mesh.shape["pcol"]),
        mesh=mesh,
        in_specs=in_specs,
        out_specs=out_specs,
        check_vma=False,
    )
```

```python
import functools
import math

import jax
import jax.numpy as jnp
from jax import lax
from jax.experimental import pallas as pl
from jax.experimental.pallas import tpu as pltpu
from jax.sharding import PartitionSpec as P

MESH = pl.DeviceIdType.MESH
LOG2E = math.log2(math.e)
F32 = jnp.float32
BF16 = jnp.bfloat16
HIGH = lax.Precision.HIGHEST


def dot(a, b, da, db, precision=None):
    return lax.dot_general(
        a, b, (((da,), (db,)), ((), ())), preferred_element_type=F32, precision=precision
    )


def split(x):
    high = x.astype(BF16)
    return high, (x - high.astype(F32)).astype(BF16)


def all_sum(x):
    return jnp.sum(jnp.sum(x, axis=1, keepdims=True), axis=0, keepdims=True)


def invert(mats):
    size = mats[0].shape[0]
    row_at = lax.broadcasted_iota(jnp.int32, (size, size), 0)
    col_at = lax.broadcasted_iota(jnp.int32, (size, size), 1)
    for k in range(size):
        following = []
        for m in mats:
            col = jnp.broadcast_to(m[:, k : k + 1], (size, size))
            inverse = 1.0 / col[k : k + 1, :]
            row = jnp.where(col_at[:1] == k, 1.0, m[k : k + 1, :]) * inverse
            rest = jnp.where(col_at == k, 0.0, m) - col * row
            following.append(jnp.where(row_at == k, row, rest))
        mats = following
    return mats


def kernel(
    rows,
    cols,
    row_tiles,
    col_tiles,
    range_length,
    smoothness,
    points_hbm,
    bank_hbm,
    ids_hbm,
    ranks_hbm,
    y_out,
    c_out,
    residuals,
    whole_out,
    points,
    ids,
    ranks,
    all_points,
    all_bank,
    low,
    norms,
    mine,
    col_sums,
    partial,
    row_sums,
    sem_local,
    sem_ps,
    sem_pr,
    sem_bs,
    sem_br,
    sem_cs,
    sem_cr,
    sem_rs,
    sem_rr,
):
    p = lax.axis_index("prow")
    q = lax.axis_index("pcol")
    per_bank, sketch_rows, size = bank_hbm.shape
    slots = [(a, b) for a in range(row_tiles) for b in range(col_tiles)]
    sibling = q + 1 - 2 * lax.rem(q, 2)

    barrier = pltpu.get_barrier_semaphore()
    for step in range(1, cols):
        pl.semaphore_signal(
            barrier, device_id=(p, lax.rem(q + step, cols)), device_id_type=MESH
        )
    for step in range(1, rows):
        pl.semaphore_signal(
            barrier, device_id=(lax.rem(p + step, rows), q), device_id_type=MESH
        )
    local = [
        pltpu.make_async_copy(source, target, sem_local.at[index])
        for index, (source, target) in enumerate(
            [
                (points_hbm, points),
                (ids_hbm, ids),
                (ranks_hbm, ranks),
                (points_hbm.at[:, 0], all_points.at[q]),
                (bank_hbm, all_bank.at[pl.ds(q * per_bank, per_bank)]),
            ]
        )
    ]
    for copy in local:
        copy.start()
    needed = q < 0
    for a in range(row_tiles):
        needed = needed | (lax.rem(a * rows + p, cols) == q)
    pl.semaphore_wait(barrier, cols + rows - 2)

    def point_copy(source, target):
        return pltpu.make_async_remote_copy(
            src_ref=points_hbm.at[:, 0],
            dst_ref=all_points.at[source],
            send_sem=sem_ps.at[target],
            recv_sem=sem_pr.at[source],
            device_id=(p, target),
            device_id_type=MESH,
        )

    def bank_copy(block, target, send):
        return pltpu.make_async_remote_copy(
            src_ref=all_bank.at[pl.ds(block * per_bank, per_bank)] if send >= cols else bank_hbm,
            dst_ref=all_bank.at[pl.ds(block * per_bank, per_bank)],
            send_sem=sem_bs.at[send],
            recv_sem=sem_br.at[block],
            device_id=(p, target),
            device_id_type=MESH,
        )

    @pl.when(needed)
    def _():
        for step in range(1, cols):
            point_copy(q, lax.rem(q + step, cols)).start()

    for step in range(2, cols, 2):
        bank_copy(q, lax.rem(q + step, cols), step).start()
    bank_copy(q, sibling, 1).start()

    for copy in local[:-1]:
        copy.wait()
    degree = jnp.full((8, 128), smoothness[0].astype(F32))
    scale = (LOG2E * jnp.sqrt(2.0 * degree + 1.0)) / jnp.full((8, 128), range_length[0])
    scale = scale[:1]
    linear = jnp.where(smoothness[0] >= 1, 1.0 / LOG2E, 0.0).astype(F32)
    square = jnp.where(smoothness[0] >= 2, 1.0 / (3.0 * LOG2E * LOG2E), 0.0).astype(F32)

    def place(slot):
        a, b = slots[slot]
        return a * rows + p, b * cols + q

    arrived = []

    def generate(slot):
        i, j = place(slot)
        a = slots[slot][0]
        owner = lax.rem(a * rows + p, cols)
        fresh = owner != q
        for before in arrived:
            if before != a:
                fresh = fresh & (owner != lax.rem(before * rows + p, cols))
        if a not in arrived:
            arrived.append(a)

            @pl.when(fresh)
            def _():
                point_copy(owner, q).wait_recv()

        @pl.when(j > i)
        def _():
            norms[slot] = jnp.zeros((8, 128), F32)

        @pl.when(j <= i)
        def _():
            row_block = lax.rem(i, cols)
            row_major = i // cols
            col_major = slots[slot][1]

            def chunk(c, total):
                at = pl.ds(pl.multiple_of(c * 128, 128), 128)
                x_row = all_points[row_block, row_major, 0:1, at] * scale
                y_row = all_points[row_block, row_major, 1:2, at] * scale
                x_row = jnp.broadcast_to(x_row, (128, 128)).T
                y_row = jnp.broadcast_to(y_row, (128, 128)).T
                for n in range(size // 128):
                    cut = slice(n * 128, n * 128 + 128)
                    x_col = points[col_major, 0, 0:1, cut] * scale
                    y_col = points[col_major, 0, 1:2, cut] * scale
                    dx = x_row - x_col
                    dy = y_row - y_col
                    d2 = dx * dx + dy * dy
                    t = d2 * lax.rsqrt(jnp.maximum(d2, 1e-30))
                    tile = (1.0 + linear * t + square * d2) * jnp.exp2(-t)
                    low[slot, at, cut] = tile.astype(BF16)
                    total = total + jnp.sum((tile * tile).reshape(16, 8, 128), axis=0)
                return total

            norms[slot] = lax.fori_loop(0, size // 128, chunk, jnp.zeros((8, 128), F32))

    generate(0)
    for step in range(2, cols, 2):
        block = lax.rem(q + step, cols)
        bank_copy(block, q, 0).wait_recv()
        bank_copy(block, sibling, cols + step).start()
    for slot in range(1, len(slots)):
        generate(slot)

    def row_copy(source, target):
        return pltpu.make_async_remote_copy(
            src_ref=mine,
            dst_ref=row_sums.at[source],
            send_sem=sem_rs.at[target],
            recv_sem=sem_rr.at[source],
            device_id=(target, q),
            device_id_type=MESH,
        )

    def col_copy(source, target):
        return pltpu.make_async_remote_copy(
            src_ref=partial,
            dst_ref=col_sums.at[source],
            send_sem=sem_cs.at[target],
            recv_sem=sem_cr.at[source],
            device_id=(p, target),
            device_id_type=MESH,
        )

    norm_sum = jnp.zeros((1, 1), F32)
    rank_sum = jnp.float32(0)
    for slot, (a, b) in enumerate(slots):
        i, j = place(slot)
        weight = jnp.where(j < i, 2.0, 1.0).astype(F32)
        norm_sum = norm_sum + weight * all_sum(norms[slot])
        rank_sum = rank_sum + jnp.where(j < i, ranks[0, b, 0, a], 0).astype(F32)
    first = lax.broadcasted_iota(jnp.int32, (8, 128), 0) == 0
    mine[...] = jnp.where(first, jnp.broadcast_to(norm_sum, (8, 128)), rank_sum)

    local[-1].wait()
    bank_copy(sibling, q, 0).wait_recv()
    for step in range(2, cols, 2):
        bank_copy(lax.rem(sibling + step, cols), q, 0).wait_recv()

    def keep_of(a, b):
        return lax.broadcasted_iota(jnp.int32, (sketch_rows, 1), 0) < ranks[0, b, 0, a]

    for slot, (a, b) in enumerate(slots):
        i, j = place(slot)
        if slot == 0:
            for step in range(1, rows):
                row_copy(p, lax.rem(p + step, rows)).start()

        @pl.when(j < i)
        def _():
            sketch = all_bank[ids[0, b, 0, a]]
            sketch = jnp.where(keep_of(a, b), sketch.astype(F32), 0.0).astype(BF16)
            y_out[a, 0, b, 0] = dot(sketch, low[slot], 1, 1)

        @pl.when(j >= i)
        def _():
            y_out[a, 0, b, 0] = jnp.zeros((sketch_rows, size), F32)
            c_out[a, 0, b, 0] = jnp.zeros((sketch_rows, size), F32)
            residuals[slot] = norms[slot]

    eye = lax.broadcasted_iota(jnp.int32, (sketch_rows, sketch_rows), 0) == (
        lax.broadcasted_iota(jnp.int32, (sketch_rows, sketch_rows), 1)
    )
    grams = []
    for slot, (a, b) in enumerate(slots):
        i, j = place(slot)
        y = y_out[a, 0, b, 0]
        gram = dot(y, y, 1, 1, HIGH)
        rank = jnp.full((1, 1), ranks[0, b, 0, a].astype(F32))
        shift = 0.1 * all_sum(jnp.where(eye, gram, 0.0)) / rank
        diagonal = jnp.where(keep_of(a, b) & (j < i), shift, 1.0)
        grams.append(gram + jnp.where(eye, diagonal, 0.0))
    inverses = invert(grams)

    summed = mine[...]
    for step in range(1, rows):
        source = lax.rem(p + step, rows)
        row_copy(source, p).wait_recv()
        summed = summed + row_sums[source]
    partial[...] = summed

    for slot, (a, b) in enumerate(slots):
        i, j = place(slot)

        @pl.when(j < i)
        def _():
            product = dot(y_out[a, 0, b, 0].astype(BF16), low[slot], 1, 0)
            c_out[a, 0, b, 0] = dot(inverses[slot], product, 1, 0, HIGH)

    for step in range(1, cols):
        col_copy(q, lax.rem(q + step, cols)).start()

    for slot, (a, b) in enumerate(slots):
        i, j = place(slot)

        @pl.when(j < i)
        def _():
            y_high, y_low = split(y_out[a, 0, b, 0])
            c_high, c_low = split(c_out[a, 0, b, 0])
            left = jnp.concatenate([y_high, y_high, y_low], axis=0)
            right = jnp.concatenate([c_high, c_low, c_high], axis=0)
            total = jnp.zeros((8, 128), F32)
            for m in range(size // 128):
                cut = slice(m * 128, m * 128 + 128)
                gap = low[slot, cut].astype(F32) - dot(left[:, cut], right, 0, 0)
                gap = gap * gap
                for n in range(size // 128):
                    total = total + jnp.sum(
                        gap[:, n * 128 : n * 128 + 128].reshape(16, 8, 128), axis=0
                    )
            residuals[slot] = total

    whole = partial[...]
    for step in range(1, cols):
        source = lax.rem(q + step, cols)
        col_copy(source, q).wait_recv()
        whole = whole + col_sums[source]
    whole_out[...] = whole

    for step in range(1, cols):
        col_copy(q, lax.rem(q + step, cols)).wait_send()

    @pl.when(needed)
    def _():
        for step in range(1, cols):
            point_copy(q, lax.rem(q + step, cols)).wait_send()

    for step in range(2, cols, 2):
        bank_copy(q, lax.rem(q + step, cols), step).wait_send()
        bank_copy(lax.rem(q + step, cols), sibling, cols + step).wait_send()
    bank_copy(q, sibling, 1).wait_send()
    for step in range(1, rows):
        row_copy(p, lax.rem(p + step, rows)).wait_send()


def finish(rows, cols, row_tiles, col_tiles, y, c, residuals, whole, y_out, c_out, err_out, rank_out, sems):
    p = lax.axis_index("prow")
    q = lax.axis_index("pcol")
    copies = [
        pltpu.make_async_copy(y, y_out, sems.at[0]),
        pltpu.make_async_copy(c, c_out, sems.at[1]),
    ]
    for copy in copies:
        copy.start()
    norm = lax.rsqrt(whole[0:1, :]) * float(cols * col_tiles)
    lane = lax.broadcasted_iota(jnp.int32, (1, 128), 1)
    for b in range(col_tiles):
        line = jnp.zeros((1, 128), F32)
        for a in range(row_tiles):
            error = jnp.sqrt(all_sum(residuals[a * col_tiles + b])) * norm
            shown = (lane == a) & (b * cols + q <= a * rows + p)
            line = jnp.where(shown, error, line)
        err_out[0, b, 0:1, :] = line[:, :row_tiles]
    rank_out[0] = whole[1:2, 0:1].astype(jnp.int32)[0, 0]
    for copy in copies:
        copy.wait()


def per_device(rows, cols, points, range_length, smoothness, bank, ids, ranks):
    row_tiles, col_tiles = ids.shape[0], ids.shape[2]
    per_bank, sketch_rows, size = bank.shape
    slots = row_tiles * col_tiles
    ids = ids.transpose(1, 2, 3, 0)
    ranks = ranks.transpose(1, 2, 3, 0)
    factors = jax.ShapeDtypeStruct((row_tiles, 1, col_tiles, 1, sketch_rows, size), F32)
    vmem = pl.BlockSpec(memory_space=pltpu.VMEM)
    smem = pl.BlockSpec(memory_space=pltpu.SMEM)
    hbm = pl.BlockSpec(memory_space=pltpu.HBM)
    dma = pltpu.SemaphoreType.DMA
    pinned = [pltpu.with_memory_space_constraint(x, pltpu.HBM) for x in (points, bank, ids, ranks)]
    y, c, residuals, whole = pl.pallas_call(
        functools.partial(kernel, rows, cols, row_tiles, col_tiles),
        out_shape=(
            factors,
            factors,
            jax.ShapeDtypeStruct((slots, 8, 128), F32),
            jax.ShapeDtypeStruct((8, 128), F32),
        ),
        in_specs=[smem, smem, hbm, hbm, hbm, hbm],
        out_specs=(vmem,) * 4,
        scratch_shapes=[
            pltpu.VMEM(points.shape, F32),
            pltpu.SMEM(ids.shape, jnp.int32),
            pltpu.SMEM(ranks.shape, jnp.int32),
            pltpu.VMEM((cols, col_tiles, 2, size), F32),
            pltpu.VMEM((cols * per_bank, sketch_rows, size), BF16),
            pltpu.VMEM((slots, size, size), BF16),
            pltpu.VMEM((slots, 8, 128), F32),
            pltpu.VMEM((8, 128), F32),
            pltpu.VMEM((cols, 8, 128), F32),
            pltpu.VMEM((8, 128), F32),
            pltpu.VMEM((rows, 8, 128), F32),
            dma((5,)),
            dma((cols,)),
            dma((cols,)),
            dma((2 * cols,)),
            dma((cols,)),
            dma((cols,)),
            dma((cols,)),
            dma((rows,)),
            dma((rows,)),
        ],
        compiler_params=pltpu.CompilerParams(
            collective_id=0, has_side_effects=True, vmem_limit_bytes=40 * 1024 * 1024
        ),
        name="tiles",
    )(range_length, smoothness, *pinned)
    y, c, errors, rank_total = pl.pallas_call(
        functools.partial(finish, rows, cols, row_tiles, col_tiles),
        out_shape=(
            factors,
            factors,
            jax.ShapeDtypeStruct((1, col_tiles, 1, row_tiles), F32),
            jax.ShapeDtypeStruct((1,), jnp.int32),
        ),
        in_specs=[vmem] * 4,
        out_specs=(hbm, hbm, vmem, smem),
        scratch_shapes=[dma((2,))],
        compiler_params=pltpu.CompilerParams(vmem_limit_bytes=16 * 1024 * 1024),
        name="finish",
    )(y, c, residuals, whole)
    return y, c, errors.transpose(3, 0, 1, 2), rank_total


def solution(mesh):
    in_specs = (
        P(None, "pcol", None, None),
        P(),
        P(),
        P("pcol", None, None),
        P(None, "prow", None, "pcol"),
        P(None, "prow", None, "pcol"),
    )
    out_specs = (
        P(None, "prow", None, "pcol", None, None),
        P(None, "prow", None, "pcol", None, None),
        P(None, "prow", None, "pcol"),
        P(),
    )
    return jax.shard_map(
        functools.partial(per_device, mesh.shape["prow"], mesh.shape["pcol"]),
        mesh=mesh,
        in_specs=in_specs,
        out_specs=out_specs,
        check_vma=False,
    )
```

```python
import functools
import math

import jax
import jax.numpy as jnp
from jax import lax
from jax.experimental import pallas as pl
from jax.experimental.pallas import tpu as pltpu
from jax.sharding import PartitionSpec as P

MESH = pl.DeviceIdType.MESH
LOG2E = math.log2(math.e)
F32 = jnp.float32
BF16 = jnp.bfloat16
HIGH = lax.Precision.HIGHEST


def dot(a, b, da, db, precision=None):
    return lax.dot_general(
        a, b, (((da,), (db,)), ((), ())), preferred_element_type=F32, precision=precision
    )


def split(x):
    high = x.astype(BF16)
    return high, (x - high.astype(F32)).astype(BF16)


def all_sum(x):
    return jnp.sum(jnp.sum(x, axis=1, keepdims=True), axis=0, keepdims=True)


def invert(mats):
    size = mats[0].shape[0]
    row_at = lax.broadcasted_iota(jnp.int32, (size, size), 0)
    col_at = lax.broadcasted_iota(jnp.int32, (size, size), 1)
    for k in range(size):
        following = []
        for m in mats:
            col = jnp.broadcast_to(m[:, k : k + 1], (size, size))
            inverse = 1.0 / col[k : k + 1, :]
            row = jnp.where(col_at[:1] == k, 1.0, m[k : k + 1, :]) * inverse
            rest = jnp.where(col_at == k, 0.0, m) - col * row
            following.append(jnp.where(row_at == k, row, rest))
        mats = following
    return mats


def kernel(
    rows,
    cols,
    row_tiles,
    col_tiles,
    range_length,
    smoothness,
    points_hbm,
    bank_hbm,
    ids_hbm,
    ranks_hbm,
    y_out,
    c_out,
    residuals,
    whole_out,
    points,
    ids,
    ranks,
    all_points,
    all_bank,
    low,
    norms,
    mine,
    sums,
    sem_local,
    sem_ps,
    sem_pr,
    sem_bs,
    sem_br,
    sem_ns,
    sem_nr,
    ready,
):
    p = lax.axis_index("prow")
    q = lax.axis_index("pcol")
    per_bank, sketch_rows, size = bank_hbm.shape
    slots = [(a, b) for a in range(row_tiles) for b in range(col_tiles)]
    sibling = q + 1 - 2 * lax.rem(q, 2)

    barrier = pltpu.get_barrier_semaphore()
    for step in range(1, cols):
        pl.semaphore_signal(
            barrier, device_id=(p, lax.rem(q + step, cols)), device_id_type=MESH
        )
    for step in range(1, rows):
        pl.semaphore_signal(
            barrier, device_id=(lax.rem(p + step, rows), q), device_id_type=MESH
        )
    local = [
        pltpu.make_async_copy(source, target, sem_local.at[index])
        for index, (source, target) in enumerate(
            [
                (points_hbm, points),
                (ids_hbm, ids),
                (ranks_hbm, ranks),
                (points_hbm.at[:, 0], all_points.at[q]),
                (bank_hbm, all_bank.at[pl.ds(q * per_bank, per_bank)]),
            ]
        )
    ]
    for copy in local:
        copy.start()
    needed = q < 0
    for a in range(row_tiles):
        needed = needed | (lax.rem(a * rows + p, cols) == q)
    pl.semaphore_wait(barrier, cols + rows - 2)
    for step in range(1, rows):
        pl.semaphore_signal(
            ready, device_id=(lax.rem(p + step, rows), q), device_id_type=MESH
        )

    def point_copy(source, target):
        return pltpu.make_async_remote_copy(
            src_ref=points_hbm.at[:, 0],
            dst_ref=all_points.at[source],
            send_sem=sem_ps.at[target],
            recv_sem=sem_pr.at[source],
            device_id=(p, target),
            device_id_type=MESH,
        )

    def bank_copy(block, target, send):
        return pltpu.make_async_remote_copy(
            src_ref=all_bank.at[pl.ds(block * per_bank, per_bank)] if send >= cols else bank_hbm,
            dst_ref=all_bank.at[pl.ds(block * per_bank, per_bank)],
            send_sem=sem_bs.at[send],
            recv_sem=sem_br.at[block],
            device_id=(p, target),
            device_id_type=MESH,
        )

    @pl.when(needed)
    def _():
        for step in range(1, cols):
            point_copy(q, lax.rem(q + step, cols)).start()

    for step in range(2, cols, 2):
        bank_copy(q, lax.rem(q + step, cols), step).start()
    bank_copy(q, sibling, 1).start()

    for copy in local[:-1]:
        copy.wait()
    degree = jnp.full((8, 128), smoothness[0].astype(F32))
    scale = (LOG2E * jnp.sqrt(2.0 * degree + 1.0)) / jnp.full((8, 128), range_length[0])
    scale = scale[:1]
    linear = jnp.where(smoothness[0] >= 1, 1.0 / LOG2E, 0.0).astype(F32)
    square = jnp.where(smoothness[0] >= 2, 1.0 / (3.0 * LOG2E * LOG2E), 0.0).astype(F32)

    def place(slot):
        a, b = slots[slot]
        return a * rows + p, b * cols + q

    arrived = []

    def generate(slot):
        i, j = place(slot)
        a = slots[slot][0]
        owner = lax.rem(a * rows + p, cols)
        fresh = owner != q
        for before in arrived:
            if before != a:
                fresh = fresh & (owner != lax.rem(before * rows + p, cols))
        if a not in arrived:
            arrived.append(a)

            @pl.when(fresh)
            def _():
                point_copy(owner, q).wait_recv()

        @pl.when(j > i)
        def _():
            norms[slot] = jnp.zeros((8, 128), F32)

        @pl.when(j <= i)
        def _():
            row_block = lax.rem(i, cols)
            row_major = i // cols
            col_major = slots[slot][1]

            def chunk(c, total):
                at = pl.ds(pl.multiple_of(c * 128, 128), 128)
                x_row = all_points[row_block, row_major, 0:1, at] * scale
                y_row = all_points[row_block, row_major, 1:2, at] * scale
                x_row = jnp.broadcast_to(x_row, (128, 128)).T
                y_row = jnp.broadcast_to(y_row, (128, 128)).T
                for n in range(size // 128):
                    cut = slice(n * 128, n * 128 + 128)
                    x_col = points[col_major, 0, 0:1, cut] * scale
                    y_col = points[col_major, 0, 1:2, cut] * scale
                    dx = x_row - x_col
                    dy = y_row - y_col
                    d2 = dx * dx + dy * dy
                    t = d2 * lax.rsqrt(jnp.maximum(d2, 1e-30))
                    tile = (1.0 + linear * t + square * d2) * jnp.exp2(-t)
                    low[slot, at, cut] = tile.astype(BF16)
                    total = total + jnp.sum((tile * tile).reshape(16, 8, 128), axis=0)
                return total

            norms[slot] = lax.fori_loop(0, size // 128, chunk, jnp.zeros((8, 128), F32))

    generate(0)
    for step in range(2, cols, 2):
        block = lax.rem(q + step, cols)
        bank_copy(block, q, 0).wait_recv()
        bank_copy(block, sibling, cols + step).start()
    for slot in range(1, len(slots)):
        generate(slot)

    devices = rows * cols
    me = p * cols + q

    def norm_copy(source, target):
        return pltpu.make_async_remote_copy(
            src_ref=mine,
            dst_ref=sums.at[source],
            send_sem=sem_ns.at[target],
            recv_sem=sem_nr.at[source],
            device_id=(target // cols, lax.rem(target, cols)),
            device_id_type=MESH,
        )

    norm_sum = jnp.zeros((1, 1), F32)
    rank_sum = jnp.float32(0)
    for slot, (a, b) in enumerate(slots):
        i, j = place(slot)
        weight = jnp.where(j < i, 2.0, 1.0).astype(F32)
        norm_sum = norm_sum + weight * all_sum(norms[slot])
        rank_sum = rank_sum + jnp.where(j < i, ranks[0, b, 0, a], 0).astype(F32)
    first = lax.broadcasted_iota(jnp.int32, (1, 128), 1) == 0
    mine[...] = jnp.where(first, jnp.broadcast_to(norm_sum, (1, 128)), rank_sum)

    local[-1].wait()
    bank_copy(sibling, q, 0).wait_recv()
    for step in range(2, cols, 2):
        bank_copy(lax.rem(sibling + step, cols), q, 0).wait_recv()

    pl.semaphore_wait(ready, rows - 1)
    for step in range(1, devices):
        norm_copy(me, lax.rem(me + step, devices)).start()

    def keep_of(a, b):
        return lax.broadcasted_iota(jnp.int32, (sketch_rows, 1), 0) < ranks[0, b, 0, a]

    for slot, (a, b) in enumerate(slots):
        i, j = place(slot)

        @pl.when(j < i)
        def _():
            sketch = all_bank[ids[0, b, 0, a]]
            sketch = jnp.where(keep_of(a, b), sketch.astype(F32), 0.0).astype(BF16)
            y_out[a, 0, b, 0] = dot(sketch, low[slot], 1, 1)

        @pl.when(j >= i)
        def _():
            y_out[a, 0, b, 0] = jnp.zeros((sketch_rows, size), F32)
            c_out[a, 0, b, 0] = jnp.zeros((sketch_rows, size), F32)
            residuals[slot] = norms[slot]

    eye = lax.broadcasted_iota(jnp.int32, (sketch_rows, sketch_rows), 0) == (
        lax.broadcasted_iota(jnp.int32, (sketch_rows, sketch_rows), 1)
    )
    grams = []
    for slot, (a, b) in enumerate(slots):
        i, j = place(slot)
        y = y_out[a, 0, b, 0]
        gram = dot(y, y, 1, 1, HIGH)
        rank = jnp.full((1, 1), ranks[0, b, 0, a].astype(F32))
        shift = 0.1 * all_sum(jnp.where(eye, gram, 0.0)) / rank
        diagonal = jnp.where(keep_of(a, b) & (j < i), shift, 1.0)
        grams.append(gram + jnp.where(eye, diagonal, 0.0))
    inverses = invert(grams)

    for slot, (a, b) in enumerate(slots):
        i, j = place(slot)

        @pl.when(j < i)
        def _():
            product = dot(y_out[a, 0, b, 0].astype(BF16), low[slot], 1, 0)
            c_out[a, 0, b, 0] = dot(inverses[slot], product, 1, 0, HIGH)

    for slot, (a, b) in enumerate(slots):
        i, j = place(slot)

        @pl.when(j < i)
        def _():
            y_high, y_low = split(y_out[a, 0, b, 0])
            c_high, c_low = split(c_out[a, 0, b, 0])
            left = jnp.concatenate([y_high, y_high, y_low], axis=0)
            right = jnp.concatenate([c_high, c_low, c_high], axis=0)
            total = jnp.zeros((8, 128), F32)
            for m in range(size // 128):
                cut = slice(m * 128, m * 128 + 128)
                gap = low[slot, cut].astype(F32) - dot(left[:, cut], right, 0, 0)
                gap = gap * gap
                for n in range(size // 128):
                    total = total + jnp.sum(
                        gap[:, n * 128 : n * 128 + 128].reshape(16, 8, 128), axis=0
                    )
            residuals[slot] = total

    whole = mine[...]
    for step in range(1, devices):
        source = lax.rem(me + step, devices)
        norm_copy(source, me).wait_recv()
        whole = whole + sums[source]
    whole_out[...] = whole

    for step in range(1, devices):
        norm_copy(me, lax.rem(me + step, devices)).wait_send()

    @pl.when(needed)
    def _():
        for step in range(1, cols):
            point_copy(q, lax.rem(q + step, cols)).wait_send()

    for step in range(2, cols, 2):
        bank_copy(q, lax.rem(q + step, cols), step).wait_send()
        bank_copy(lax.rem(q + step, cols), sibling, cols + step).wait_send()
    bank_copy(q, sibling, 1).wait_send()


def finish(rows, cols, row_tiles, col_tiles, y, c, residuals, whole, y_out, c_out, err_out, rank_out, sems):
    p = lax.axis_index("prow")
    q = lax.axis_index("pcol")
    copies = [
        pltpu.make_async_copy(y, y_out, sems.at[0]),
        pltpu.make_async_copy(c, c_out, sems.at[1]),
    ]
    for copy in copies:
        copy.start()
    norm = lax.rsqrt(whole[0:1, 0:1]) * float(cols * col_tiles)
    lane = lax.broadcasted_iota(jnp.int32, (1, 128), 1)
    for b in range(col_tiles):
        line = jnp.zeros((1, 128), F32)
        for a in range(row_tiles):
            error = jnp.sqrt(all_sum(residuals[a * col_tiles + b])) * norm
            shown = (lane == a) & (b * cols + q <= a * rows + p)
            line = jnp.where(shown, error, line)
        err_out[0, b, 0:1, :] = line[:, :row_tiles]
    rank_out[0] = whole[0:1, 1:2].astype(jnp.int32)[0, 0]
    for copy in copies:
        copy.wait()


def per_device(rows, cols, points, range_length, smoothness, bank, ids, ranks):
    row_tiles, col_tiles = ids.shape[0], ids.shape[2]
    per_bank, sketch_rows, size = bank.shape
    slots = row_tiles * col_tiles
    ids = ids.transpose(1, 2, 3, 0)
    ranks = ranks.transpose(1, 2, 3, 0)
    factors = jax.ShapeDtypeStruct((row_tiles, 1, col_tiles, 1, sketch_rows, size), F32)
    vmem = pl.BlockSpec(memory_space=pltpu.VMEM)
    smem = pl.BlockSpec(memory_space=pltpu.SMEM)
    hbm = pl.BlockSpec(memory_space=pltpu.HBM)
    dma = pltpu.SemaphoreType.DMA
    pinned = [pltpu.with_memory_space_constraint(x, pltpu.HBM) for x in (points, bank, ids, ranks)]
    y, c, residuals, whole = pl.pallas_call(
        functools.partial(kernel, rows, cols, row_tiles, col_tiles),
        out_shape=(
            factors,
            factors,
            jax.ShapeDtypeStruct((slots, 8, 128), F32),
            jax.ShapeDtypeStruct((1, 128), F32),
        ),
        in_specs=[smem, smem, hbm, hbm, hbm, hbm],
        out_specs=(vmem,) * 4,
        scratch_shapes=[
            pltpu.VMEM(points.shape, F32),
            pltpu.SMEM(ids.shape, jnp.int32),
            pltpu.SMEM(ranks.shape, jnp.int32),
            pltpu.VMEM((cols, col_tiles, 2, size), F32),
            pltpu.VMEM((cols * per_bank, sketch_rows, size), BF16),
            pltpu.VMEM((slots, size, size), BF16),
            pltpu.VMEM((slots, 8, 128), F32),
            pltpu.VMEM((1, 128), F32),
            pltpu.VMEM((rows * cols, 1, 128), F32),
            dma((5,)),
            dma((cols,)),
            dma((cols,)),
            dma((2 * cols,)),
            dma((cols,)),
            dma((rows * cols,)),
            dma((rows * cols,)),
            pltpu.SemaphoreType.REGULAR,
        ],
        compiler_params=pltpu.CompilerParams(
            collective_id=0, has_side_effects=True, vmem_limit_bytes=40 * 1024 * 1024
        ),
        name="tiles",
    )(range_length, smoothness, *pinned)
    y, c, errors, rank_total = pl.pallas_call(
        functools.partial(finish, rows, cols, row_tiles, col_tiles),
        out_shape=(
            factors,
            factors,
            jax.ShapeDtypeStruct((1, col_tiles, 1, row_tiles), F32),
            jax.ShapeDtypeStruct((1,), jnp.int32),
        ),
        in_specs=[vmem] * 4,
        out_specs=(hbm, hbm, vmem, smem),
        scratch_shapes=[dma((2,))],
        compiler_params=pltpu.CompilerParams(vmem_limit_bytes=16 * 1024 * 1024),
        name="finish",
    )(y, c, residuals, whole)
    return y, c, errors.transpose(3, 0, 1, 2), rank_total


def solution(mesh):
    in_specs = (
        P(None, "pcol", None, None),
        P(),
        P(),
        P("pcol", None, None),
        P(None, "prow", None, "pcol"),
        P(None, "prow", None, "pcol"),
    )
    out_specs = (
        P(None, "prow", None, "pcol", None, None),
        P(None, "prow", None, "pcol", None, None),
        P(None, "prow", None, "pcol"),
        P(),
    )
    return jax.shard_map(
        functools.partial(per_device, mesh.shape["prow"], mesh.shape["pcol"]),
        mesh=mesh,
        in_specs=in_specs,
        out_specs=out_specs,
        check_vma=False,
    )
```

```python
import functools
import math

import jax
import jax.numpy as jnp
from jax import lax
from jax.experimental import pallas as pl
from jax.experimental.pallas import tpu as pltpu
from jax.sharding import PartitionSpec as P

MESH = pl.DeviceIdType.MESH
LOG2E = math.log2(math.e)
F32 = jnp.float32
BF16 = jnp.bfloat16
HIGH = lax.Precision.HIGHEST


def dot(a, b, da, db, precision=None):
    return lax.dot_general(
        a, b, (((da,), (db,)), ((), ())), preferred_element_type=F32, precision=precision
    )


def split(x):
    high = x.astype(BF16)
    return high, (x - high.astype(F32)).astype(BF16)


def all_sum(x):
    return jnp.sum(jnp.sum(x, axis=1, keepdims=True), axis=0, keepdims=True)


def invert(mats, group=8):
    size = mats[0].shape[0]
    parts = size // 8
    sub = lax.broadcasted_iota(jnp.int32, (8, size), 0)
    lane = lax.broadcasted_iota(jnp.int32, (8, size), 1)
    mats = [[m[8 * v : 8 * v + 8] for v in range(parts)] for m in mats]
    for start in range(0, size, group):
        spread = [
            {
                k: [jnp.broadcast_to(part[:, k : k + 1], (8, size)) for part in m]
                for k in range(start, start + group)
            }
            for m in mats
        ]
        for k in range(start, start + group):
            at, within = divmod(k, 8)
            for index, (m, cols) in enumerate(zip(mats, spread)):
                col = cols.pop(k)
                pivot = jnp.broadcast_to(col[at][within : within + 1], (8, size))
                inverse = 1.0 / pivot
                for other, entry in cols.items():
                    head = jnp.broadcast_to(entry[at][within : within + 1], (8, size)) * inverse
                    entry = [e - c * head for e, c in zip(entry, col)]
                    entry[at] = jnp.where(sub == within, head, entry[at])
                    cols[other] = entry
                row = jnp.broadcast_to(m[at][within : within + 1], (8, size))
                row = jnp.where(lane == k, 1.0, row) * inverse
                m = [jnp.where(lane == k, 0.0, part) - c * row for part, c in zip(m, col)]
                m[at] = jnp.where(sub == within, row, m[at])
                mats[index] = m
    return [jnp.concatenate(m, axis=0) for m in mats]


def kernel(
    rows,
    cols,
    row_tiles,
    col_tiles,
    range_length,
    smoothness,
    points_hbm,
    bank_hbm,
    ids_hbm,
    ranks_hbm,
    y_out,
    c_out,
    residuals,
    whole_out,
    points,
    ids,
    ranks,
    all_points,
    all_bank,
    low,
    norms,
    mine,
    sums,
    sem_local,
    sem_ps,
    sem_pr,
    sem_bs,
    sem_br,
    sem_ns,
    sem_nr,
    ready,
):
    p = lax.axis_index("prow")
    q = lax.axis_index("pcol")
    per_bank, sketch_rows, size = bank_hbm.shape
    slots = [(a, b) for a in range(row_tiles) for b in range(col_tiles)]
    sibling = q + 1 - 2 * lax.rem(q, 2)

    barrier = pltpu.get_barrier_semaphore()
    for step in range(1, cols):
        pl.semaphore_signal(
            barrier, device_id=(p, lax.rem(q + step, cols)), device_id_type=MESH
        )
    for step in range(1, rows):
        pl.semaphore_signal(
            barrier, device_id=(lax.rem(p + step, rows), q), device_id_type=MESH
        )
    local = [
        pltpu.make_async_copy(source, target, sem_local.at[index])
        for index, (source, target) in enumerate(
            [
                (points_hbm, points),
                (ids_hbm, ids),
                (ranks_hbm, ranks),
                (points_hbm.at[:, 0], all_points.at[q]),
                (bank_hbm, all_bank.at[pl.ds(q * per_bank, per_bank)]),
            ]
        )
    ]
    for copy in local:
        copy.start()
    needed = q < 0
    for a in range(row_tiles):
        needed = needed | (lax.rem(a * rows + p, cols) == q)
    pl.semaphore_wait(barrier, cols + rows - 2)
    for step in range(1, rows):
        pl.semaphore_signal(
            ready, device_id=(lax.rem(p + step, rows), q), device_id_type=MESH
        )

    def point_copy(source, target):
        return pltpu.make_async_remote_copy(
            src_ref=points_hbm.at[:, 0],
            dst_ref=all_points.at[source],
            send_sem=sem_ps.at[target],
            recv_sem=sem_pr.at[source],
            device_id=(p, target),
            device_id_type=MESH,
        )

    def bank_copy(block, target, send):
        return pltpu.make_async_remote_copy(
            src_ref=all_bank.at[pl.ds(block * per_bank, per_bank)] if send >= cols else bank_hbm,
            dst_ref=all_bank.at[pl.ds(block * per_bank, per_bank)],
            send_sem=sem_bs.at[send],
            recv_sem=sem_br.at[block],
            device_id=(p, target),
            device_id_type=MESH,
        )

    @pl.when(needed)
    def _():
        for step in range(1, cols):
            point_copy(q, lax.rem(q + step, cols)).start()

    for step in range(2, cols, 2):
        bank_copy(q, lax.rem(q + step, cols), step).start()
    bank_copy(q, sibling, 1).start()

    for copy in local[:-1]:
        copy.wait()
    degree = jnp.full((8, 128), smoothness[0].astype(F32))
    scale = (LOG2E * jnp.sqrt(2.0 * degree + 1.0)) / jnp.full((8, 128), range_length[0])
    scale = scale[:1]
    linear = jnp.where(smoothness[0] >= 1, 1.0 / LOG2E, 0.0).astype(F32)
    square = jnp.where(smoothness[0] >= 2, 1.0 / (3.0 * LOG2E * LOG2E), 0.0).astype(F32)

    def place(slot):
        a, b = slots[slot]
        return a * rows + p, b * cols + q

    arrived = []

    def generate(slot):
        i, j = place(slot)
        a = slots[slot][0]
        owner = lax.rem(a * rows + p, cols)
        fresh = owner != q
        for before in arrived:
            if before != a:
                fresh = fresh & (owner != lax.rem(before * rows + p, cols))
        if a not in arrived:
            arrived.append(a)

            @pl.when(fresh)
            def _():
                point_copy(owner, q).wait_recv()

        @pl.when(j > i)
        def _():
            norms[slot] = jnp.zeros((8, 128), F32)

        @pl.when(j <= i)
        def _():
            row_block = lax.rem(i, cols)
            row_major = i // cols
            col_major = slots[slot][1]

            def chunk(c, total):
                at = pl.ds(pl.multiple_of(c * 128, 128), 128)
                x_row = all_points[row_block, row_major, 0:1, at] * scale
                y_row = all_points[row_block, row_major, 1:2, at] * scale
                x_row = jnp.broadcast_to(x_row, (128, 128)).T
                y_row = jnp.broadcast_to(y_row, (128, 128)).T
                for n in range(size // 128):
                    cut = slice(n * 128, n * 128 + 128)
                    x_col = points[col_major, 0, 0:1, cut] * scale
                    y_col = points[col_major, 0, 1:2, cut] * scale
                    dx = x_row - x_col
                    dy = y_row - y_col
                    d2 = dx * dx + dy * dy
                    t = d2 * lax.rsqrt(jnp.maximum(d2, 1e-30))
                    tile = (1.0 + linear * t + square * d2) * jnp.exp2(-t)
                    low[slot, at, cut] = tile.astype(BF16)
                    total = total + jnp.sum((tile * tile).reshape(16, 8, 128), axis=0)
                return total

            norms[slot] = lax.fori_loop(0, size // 128, chunk, jnp.zeros((8, 128), F32))

    generate(0)
    for step in range(2, cols, 2):
        block = lax.rem(q + step, cols)
        bank_copy(block, q, 0).wait_recv()
        bank_copy(block, sibling, cols + step).start()
    for slot in range(1, len(slots)):
        generate(slot)

    devices = rows * cols
    me = p * cols + q

    def norm_copy(source, target):
        return pltpu.make_async_remote_copy(
            src_ref=mine,
            dst_ref=sums.at[source],
            send_sem=sem_ns.at[target],
            recv_sem=sem_nr.at[source],
            device_id=(target // cols, lax.rem(target, cols)),
            device_id_type=MESH,
        )

    norm_sum = jnp.zeros((8, 128), F32)
    rank_sum = jnp.float32(0)
    for slot, (a, b) in enumerate(slots):
        i, j = place(slot)
        norm_sum = norm_sum + jnp.where(j < i, 2.0, 1.0).astype(F32) * norms[slot]
        rank_sum = rank_sum + jnp.where(j < i, ranks[0, b, 0, a], 0).astype(F32)
    mine[0:1, :] = jnp.sum(norm_sum, axis=0, keepdims=True)
    mine[1:2, :] = jnp.full((1, 128), rank_sum)

    pl.semaphore_wait(ready, rows - 1)
    for step in range(1, devices):
        norm_copy(me, lax.rem(me + step, devices)).start()

    local[-1].wait()
    bank_copy(sibling, q, 0).wait_recv()
    for step in range(2, cols, 2):
        bank_copy(lax.rem(sibling + step, cols), q, 0).wait_recv()

    def keep_of(a, b):
        return lax.broadcasted_iota(jnp.int32, (sketch_rows, 1), 0) < ranks[0, b, 0, a]

    for slot, (a, b) in enumerate(slots):
        i, j = place(slot)

        @pl.when(j < i)
        def _():
            sketch = all_bank[ids[0, b, 0, a]]
            sketch = jnp.where(keep_of(a, b), sketch.astype(F32), 0.0).astype(BF16)
            y_out[a, 0, b, 0] = dot(sketch, low[slot], 1, 1)

        @pl.when(j >= i)
        def _():
            y_out[a, 0, b, 0] = jnp.zeros((sketch_rows, size), F32)
            c_out[a, 0, b, 0] = jnp.zeros((sketch_rows, size), F32)
            residuals[slot] = norms[slot]

    eye = lax.broadcasted_iota(jnp.int32, (sketch_rows, sketch_rows), 0) == (
        lax.broadcasted_iota(jnp.int32, (sketch_rows, sketch_rows), 1)
    )
    grams = []
    for slot, (a, b) in enumerate(slots):
        i, j = place(slot)
        y = y_out[a, 0, b, 0]
        gram = dot(y, y, 1, 1, HIGH)
        rank = jnp.full((1, 1), ranks[0, b, 0, a].astype(F32))
        shift = 0.1 * all_sum(jnp.where(eye, gram, 0.0)) / rank
        diagonal = jnp.where(keep_of(a, b) & (j < i), shift, 1.0)
        grams.append(gram + jnp.where(eye, diagonal, 0.0))
    inverses = invert(grams)

    for slot, (a, b) in enumerate(slots):
        i, j = place(slot)

        @pl.when(j < i)
        def _():
            product = dot(y_out[a, 0, b, 0].astype(BF16), low[slot], 1, 0)
            c_out[a, 0, b, 0] = dot(inverses[slot], product, 1, 0, HIGH)

    for slot, (a, b) in enumerate(slots):
        i, j = place(slot)

        @pl.when(j < i)
        def _():
            y_high, y_low = split(y_out[a, 0, b, 0])
            c_high, c_low = split(c_out[a, 0, b, 0])
            left = jnp.concatenate([y_high, y_high, y_low], axis=0)
            right = jnp.concatenate([c_high, c_low, c_high], axis=0)
            total = jnp.zeros((8, 128), F32)
            for m in range(size // 128):
                cut = slice(m * 128, m * 128 + 128)
                gap = low[slot, cut].astype(F32) - dot(left[:, cut], right, 0, 0)
                gap = gap * gap
                for n in range(size // 128):
                    total = total + jnp.sum(
                        gap[:, n * 128 : n * 128 + 128].reshape(16, 8, 128), axis=0
                    )
            residuals[slot] = total

    whole = mine[...]
    for step in range(1, devices):
        source = lax.rem(me + step, devices)
        norm_copy(source, me).wait_recv()
        whole = whole + sums[source]
    whole_out[...] = whole

    for step in range(1, devices):
        norm_copy(me, lax.rem(me + step, devices)).wait_send()

    @pl.when(needed)
    def _():
        for step in range(1, cols):
            point_copy(q, lax.rem(q + step, cols)).wait_send()

    for step in range(2, cols, 2):
        bank_copy(q, lax.rem(q + step, cols), step).wait_send()
        bank_copy(lax.rem(q + step, cols), sibling, cols + step).wait_send()
    bank_copy(q, sibling, 1).wait_send()


def finish(rows, cols, row_tiles, col_tiles, y, c, residuals, whole, y_out, c_out, err_out, rank_out, sems):
    p = lax.axis_index("prow")
    q = lax.axis_index("pcol")
    copies = [
        pltpu.make_async_copy(y, y_out, sems.at[0]),
        pltpu.make_async_copy(c, c_out, sems.at[1]),
    ]
    for copy in copies:
        copy.start()
    norm = lax.rsqrt(all_sum(whole[0:1, :])) * float(cols * col_tiles)
    lane = lax.broadcasted_iota(jnp.int32, (1, 128), 1)
    for b in range(col_tiles):
        line = jnp.zeros((1, 128), F32)
        for a in range(row_tiles):
            error = jnp.sqrt(all_sum(residuals[a * col_tiles + b])) * norm
            shown = (lane == a) & (b * cols + q <= a * rows + p)
            line = jnp.where(shown, error, line)
        err_out[0, b, 0:1, :] = line[:, :row_tiles]
    rank_out[0] = whole[1:2, 0:1].astype(jnp.int32)[0, 0]
    for copy in copies:
        copy.wait()


def per_device(rows, cols, points, range_length, smoothness, bank, ids, ranks):
    row_tiles, col_tiles = ids.shape[0], ids.shape[2]
    per_bank, sketch_rows, size = bank.shape
    slots = row_tiles * col_tiles
    ids = ids.transpose(1, 2, 3, 0)
    ranks = ranks.transpose(1, 2, 3, 0)
    factors = jax.ShapeDtypeStruct((row_tiles, 1, col_tiles, 1, sketch_rows, size), F32)
    vmem = pl.BlockSpec(memory_space=pltpu.VMEM)
    smem = pl.BlockSpec(memory_space=pltpu.SMEM)
    hbm = pl.BlockSpec(memory_space=pltpu.HBM)
    dma = pltpu.SemaphoreType.DMA
    pinned = [pltpu.with_memory_space_constraint(x, pltpu.HBM) for x in (points, bank, ids, ranks)]
    y, c, residuals, whole = pl.pallas_call(
        functools.partial(kernel, rows, cols, row_tiles, col_tiles),
        out_shape=(
            factors,
            factors,
            jax.ShapeDtypeStruct((slots, 8, 128), F32),
            jax.ShapeDtypeStruct((2, 128), F32),
        ),
        in_specs=[smem, smem, hbm, hbm, hbm, hbm],
        out_specs=(vmem,) * 4,
        scratch_shapes=[
            pltpu.VMEM(points.shape, F32),
            pltpu.SMEM(ids.shape, jnp.int32),
            pltpu.SMEM(ranks.shape, jnp.int32),
            pltpu.VMEM((cols, col_tiles, 2, size), F32),
            pltpu.VMEM((cols * per_bank, sketch_rows, size), BF16),
            pltpu.VMEM((slots, size, size), BF16),
            pltpu.VMEM((slots, 8, 128), F32),
            pltpu.VMEM((2, 128), F32),
            pltpu.VMEM((rows * cols, 2, 128), F32),
            dma((5,)),
            dma((cols,)),
            dma((cols,)),
            dma((2 * cols,)),
            dma((cols,)),
            dma((rows * cols,)),
            dma((rows * cols,)),
            pltpu.SemaphoreType.REGULAR,
        ],
        compiler_params=pltpu.CompilerParams(
            collective_id=0, has_side_effects=True, vmem_limit_bytes=40 * 1024 * 1024
        ),
        name="tiles",
    )(range_length, smoothness, *pinned)
    y, c, errors, rank_total = pl.pallas_call(
        functools.partial(finish, rows, cols, row_tiles, col_tiles),
        out_shape=(
            factors,
            factors,
            jax.ShapeDtypeStruct((1, col_tiles, 1, row_tiles), F32),
            jax.ShapeDtypeStruct((1,), jnp.int32),
        ),
        in_specs=[vmem] * 4,
        out_specs=(hbm, hbm, vmem, smem),
        scratch_shapes=[dma((2,))],
        compiler_params=pltpu.CompilerParams(vmem_limit_bytes=16 * 1024 * 1024),
        name="finish",
    )(y, c, residuals, whole)
    return y, c, errors.transpose(3, 0, 1, 2), rank_total


def solution(mesh):
    in_specs = (
        P(None, "pcol", None, None),
        P(),
        P(),
        P("pcol", None, None),
        P(None, "prow", None, "pcol"),
        P(None, "prow", None, "pcol"),
    )
    out_specs = (
        P(None, "prow", None, "pcol", None, None),
        P(None, "prow", None, "pcol", None, None),
        P(None, "prow", None, "pcol"),
        P(),
    )
    return jax.shard_map(
        functools.partial(per_device, mesh.shape["prow"], mesh.shape["pcol"]),
        mesh=mesh,
        in_specs=in_specs,
        out_specs=out_specs,
        check_vma=False,
    )
```

```python
import functools
import math

import jax
import jax.numpy as jnp
from jax import lax
from jax.experimental import pallas as pl
from jax.experimental.pallas import tpu as pltpu
from jax.sharding import PartitionSpec as P

MESH = pl.DeviceIdType.MESH
LOG2E = math.log2(math.e)
F32 = jnp.float32
BF16 = jnp.bfloat16
HIGH = lax.Precision.HIGHEST


def dot(a, b, da, db, precision=None):
    return lax.dot_general(
        a, b, (((da,), (db,)), ((), ())), preferred_element_type=F32, precision=precision
    )


def split(x):
    high = x.astype(BF16)
    return high, (x - high.astype(F32)).astype(BF16)


def all_sum(x):
    return jnp.sum(jnp.sum(x, axis=1, keepdims=True), axis=0, keepdims=True)


def invert(mats, group=8):
    size = mats[0].shape[0]
    parts = size // 8
    sub = lax.broadcasted_iota(jnp.int32, (8, size), 0)
    lane = lax.broadcasted_iota(jnp.int32, (8, size), 1)
    mats = [[m[8 * v : 8 * v + 8] for v in range(parts)] for m in mats]
    for start in range(0, size, group):
        spread = [
            {
                k: [jnp.broadcast_to(part[:, k : k + 1], (8, size)) for part in m]
                for k in range(start, start + group)
            }
            for m in mats
        ]
        for k in range(start, start + group):
            at, within = divmod(k, 8)
            for index, (m, cols) in enumerate(zip(mats, spread)):
                col = cols.pop(k)
                pivot = jnp.broadcast_to(col[at][within : within + 1], (8, size))
                inverse = 1.0 / pivot
                for other, entry in cols.items():
                    head = jnp.broadcast_to(entry[at][within : within + 1], (8, size)) * inverse
                    entry = [e - c * head for e, c in zip(entry, col)]
                    entry[at] = jnp.where(sub == within, head, entry[at])
                    cols[other] = entry
                row = jnp.broadcast_to(m[at][within : within + 1], (8, size))
                row = jnp.where(lane == k, 1.0, row) * inverse
                m = [jnp.where(lane == k, 0.0, part) - c * row for part, c in zip(m, col)]
                m[at] = jnp.where(sub == within, row, m[at])
                mats[index] = m
    return [jnp.concatenate(m, axis=0) for m in mats]


def kernel(
    rows,
    cols,
    row_tiles,
    col_tiles,
    range_length,
    smoothness,
    points_hbm,
    bank_hbm,
    ids_hbm,
    ranks_hbm,
    y_out,
    c_out,
    residuals,
    whole_out,
    points,
    ids,
    ranks,
    all_points,
    all_bank,
    low,
    norms,
    mine,
    sums,
    sem_local,
    sem_ps,
    sem_pr,
    sem_bs,
    sem_br,
    sem_ns,
    sem_nr,
    ready,
):
    p = lax.axis_index("prow")
    q = lax.axis_index("pcol")
    per_bank, sketch_rows, size = bank_hbm.shape
    slots = [(a, b) for a in range(row_tiles) for b in range(col_tiles)]
    sibling = q + 1 - 2 * lax.rem(q, 2)

    barrier = pltpu.get_barrier_semaphore()
    for step in range(1, cols):
        pl.semaphore_signal(
            barrier, device_id=(p, lax.rem(q + step, cols)), device_id_type=MESH
        )
    for step in range(1, rows):
        pl.semaphore_signal(
            barrier, device_id=(lax.rem(p + step, rows), q), device_id_type=MESH
        )
    local = [
        pltpu.make_async_copy(source, target, sem_local.at[index])
        for index, (source, target) in enumerate(
            [
                (points_hbm, points),
                (ids_hbm, ids),
                (ranks_hbm, ranks),
                (points_hbm.at[:, 0], all_points.at[q]),
                (bank_hbm, all_bank.at[pl.ds(q * per_bank, per_bank)]),
            ]
        )
    ]
    for copy in local:
        copy.start()
    needed = q < 0
    for a in range(row_tiles):
        needed = needed | (lax.rem(a * rows + p, cols) == q)
    pl.semaphore_wait(barrier, cols + rows - 2)
    for step in range(1, rows):
        pl.semaphore_signal(
            ready, device_id=(lax.rem(p + step, rows), q), device_id_type=MESH
        )

    def point_copy(source, target):
        return pltpu.make_async_remote_copy(
            src_ref=points_hbm.at[:, 0],
            dst_ref=all_points.at[source],
            send_sem=sem_ps.at[target],
            recv_sem=sem_pr.at[source],
            device_id=(p, target),
            device_id_type=MESH,
        )

    def bank_copy(block, target, send):
        return pltpu.make_async_remote_copy(
            src_ref=all_bank.at[pl.ds(block * per_bank, per_bank)] if send >= cols else bank_hbm,
            dst_ref=all_bank.at[pl.ds(block * per_bank, per_bank)],
            send_sem=sem_bs.at[send],
            recv_sem=sem_br.at[block],
            device_id=(p, target),
            device_id_type=MESH,
        )

    @pl.when(needed)
    def _():
        for step in range(1, cols):
            point_copy(q, lax.rem(q + step, cols)).start()

    for step in range(2, cols, 2):
        bank_copy(q, lax.rem(q + step, cols), step).start()
    bank_copy(q, sibling, 1).start()

    for copy in local[:-1]:
        copy.wait()
    degree = jnp.full((8, 128), smoothness[0].astype(F32))
    scale = (LOG2E * jnp.sqrt(2.0 * degree + 1.0)) / jnp.full((8, 128), range_length[0])
    scale = scale[:1]
    linear = jnp.where(smoothness[0] >= 1, 1.0 / LOG2E, 0.0).astype(F32)
    square = jnp.where(smoothness[0] >= 2, 1.0 / (3.0 * LOG2E * LOG2E), 0.0).astype(F32)

    def place(slot):
        a, b = slots[slot]
        return a * rows + p, b * cols + q

    arrived = []

    def generate(slot, begin=0, end=size // 128):
        i, j = place(slot)
        a = slots[slot][0]
        owner = lax.rem(a * rows + p, cols)
        fresh = owner != q
        for before in arrived:
            if before != a:
                fresh = fresh & (owner != lax.rem(before * rows + p, cols))
        if a not in arrived and begin == 0:
            arrived.append(a)

            @pl.when(fresh)
            def _():
                point_copy(owner, q).wait_recv()

        @pl.when(j > i)
        def _():
            norms[slot] = jnp.zeros((8, 128), F32)

        @pl.when(j <= i)
        def _():
            row_block = lax.rem(i, cols)
            row_major = i // cols
            col_major = slots[slot][1]

            def chunk(c, total):
                at = pl.ds(pl.multiple_of(c * 128, 128), 128)
                x_row = all_points[row_block, row_major, 0:1, at] * scale
                y_row = all_points[row_block, row_major, 1:2, at] * scale
                x_row = jnp.broadcast_to(x_row, (128, 128)).T
                y_row = jnp.broadcast_to(y_row, (128, 128)).T
                for n in range(size // 128):
                    cut = slice(n * 128, n * 128 + 128)
                    x_col = points[col_major, 0, 0:1, cut] * scale
                    y_col = points[col_major, 0, 1:2, cut] * scale
                    dx = x_row - x_col
                    dy = y_row - y_col
                    d2 = dx * dx + dy * dy
                    t = d2 * lax.rsqrt(jnp.maximum(d2, 1e-30))
                    tile = (1.0 + linear * t + square * d2) * jnp.exp2(-t)
                    low[slot, at, cut] = tile.astype(BF16)
                    total = total + jnp.sum((tile * tile).reshape(16, 8, 128), axis=0)
                return total

            total = jnp.zeros((8, 128), F32) if begin == 0 else norms[slot]
            norms[slot] = lax.fori_loop(begin, end, chunk, total)

    def forward(steps):
        for step in steps:
            block = lax.rem(q + step, cols)
            bank_copy(block, q, 0).wait_recv()
            bank_copy(block, sibling, cols + step).start()

    for slot in range(len(slots) - 1):
        generate(slot)
    half = size // 256
    generate(len(slots) - 1, 0, half)
    forward(range(2, cols, 2))
    generate(len(slots) - 1, half)

    devices = rows * cols
    me = p * cols + q

    def norm_copy(source, target):
        return pltpu.make_async_remote_copy(
            src_ref=mine,
            dst_ref=sums.at[source],
            send_sem=sem_ns.at[target],
            recv_sem=sem_nr.at[source],
            device_id=(target // cols, lax.rem(target, cols)),
            device_id_type=MESH,
        )

    norm_sum = jnp.zeros((8, 128), F32)
    rank_sum = jnp.float32(0)
    for slot, (a, b) in enumerate(slots):
        i, j = place(slot)
        norm_sum = norm_sum + jnp.where(j < i, 2.0, 1.0).astype(F32) * norms[slot]
        rank_sum = rank_sum + jnp.where(j < i, ranks[0, b, 0, a], 0).astype(F32)
    mine[0:1, :] = jnp.sum(norm_sum, axis=0, keepdims=True)
    mine[1:2, :] = jnp.full((1, 128), rank_sum)

    pl.semaphore_wait(ready, rows - 1)
    for step in range(1, devices):
        norm_copy(me, lax.rem(me + step, devices)).start()

    local[-1].wait()
    bank_copy(sibling, q, 0).wait_recv()
    for step in range(2, cols, 2):
        bank_copy(lax.rem(sibling + step, cols), q, 0).wait_recv()

    def keep_of(a, b):
        return lax.broadcasted_iota(jnp.int32, (sketch_rows, 1), 0) < ranks[0, b, 0, a]

    for slot, (a, b) in enumerate(slots):
        i, j = place(slot)

        @pl.when(j < i)
        def _():
            sketch = all_bank[ids[0, b, 0, a]]
            sketch = jnp.where(keep_of(a, b), sketch.astype(F32), 0.0).astype(BF16)
            y_out[a, 0, b, 0] = dot(sketch, low[slot], 1, 1)

        @pl.when(j >= i)
        def _():
            y_out[a, 0, b, 0] = jnp.zeros((sketch_rows, size), F32)
            c_out[a, 0, b, 0] = jnp.zeros((sketch_rows, size), F32)
            residuals[slot] = norms[slot]

    eye = lax.broadcasted_iota(jnp.int32, (sketch_rows, sketch_rows), 0) == (
        lax.broadcasted_iota(jnp.int32, (sketch_rows, sketch_rows), 1)
    )
    grams = []
    for slot, (a, b) in enumerate(slots):
        i, j = place(slot)
        y = y_out[a, 0, b, 0]
        gram = dot(y, y, 1, 1, HIGH)
        rank = jnp.full((1, 1), ranks[0, b, 0, a].astype(F32))
        shift = 0.1 * all_sum(jnp.where(eye, gram, 0.0)) / rank
        diagonal = jnp.where(keep_of(a, b) & (j < i), shift, 1.0)
        grams.append(gram + jnp.where(eye, diagonal, 0.0))
    inverses = invert(grams)

    for slot, (a, b) in enumerate(slots):
        i, j = place(slot)

        @pl.when(j < i)
        def _():
            product = dot(y_out[a, 0, b, 0].astype(BF16), low[slot], 1, 0)
            c_out[a, 0, b, 0] = dot(inverses[slot], product, 1, 0, HIGH)

    for slot, (a, b) in enumerate(slots):
        i, j = place(slot)

        @pl.when(j < i)
        def _():
            y_high, y_low = split(y_out[a, 0, b, 0])
            c_high, c_low = split(c_out[a, 0, b, 0])
            left = jnp.concatenate([y_high, y_high, y_low], axis=0)
            right = jnp.concatenate([c_high, c_low, c_high], axis=0)
            total = jnp.zeros((8, 128), F32)
            for m in range(size // 128):
                cut = slice(m * 128, m * 128 + 128)
                gap = low[slot, cut].astype(F32) - dot(left[:, cut], right, 0, 0)
                gap = gap * gap
                for n in range(size // 128):
                    total = total + jnp.sum(
                        gap[:, n * 128 : n * 128 + 128].reshape(16, 8, 128), axis=0
                    )
            residuals[slot] = total

    whole = mine[...]
    for step in range(1, devices):
        source = lax.rem(me + step, devices)
        norm_copy(source, me).wait_recv()
        whole = whole + sums[source]
    whole_out[...] = whole

    for step in range(1, devices):
        norm_copy(me, lax.rem(me + step, devices)).wait_send()

    @pl.when(needed)
    def _():
        for step in range(1, cols):
            point_copy(q, lax.rem(q + step, cols)).wait_send()

    for step in range(2, cols, 2):
        bank_copy(q, lax.rem(q + step, cols), step).wait_send()
        bank_copy(lax.rem(q + step, cols), sibling, cols + step).wait_send()
    bank_copy(q, sibling, 1).wait_send()


def finish(rows, cols, row_tiles, col_tiles, y, c, residuals, whole, y_out, c_out, err_out, rank_out, sems):
    p = lax.axis_index("prow")
    q = lax.axis_index("pcol")
    copies = [
        pltpu.make_async_copy(source.at[a], target.at[a], sems.at[index, a])
        for index, (source, target) in enumerate([(y, y_out), (c, c_out)])
        for a in range(row_tiles)
    ]
    for copy in copies:
        copy.start()
    norm = lax.rsqrt(all_sum(whole[0:1, :])) * float(cols * col_tiles)
    lane = lax.broadcasted_iota(jnp.int32, (1, 128), 1)
    for b in range(col_tiles):
        line = jnp.zeros((1, 128), F32)
        for a in range(row_tiles):
            error = jnp.sqrt(all_sum(residuals[a * col_tiles + b])) * norm
            shown = (lane == a) & (b * cols + q <= a * rows + p)
            line = jnp.where(shown, error, line)
        err_out[0, b, 0:1, :] = line[:, :row_tiles]
    rank_out[0] = whole[1:2, 0:1].astype(jnp.int32)[0, 0]
    for copy in copies:
        copy.wait()


def per_device(rows, cols, points, range_length, smoothness, bank, ids, ranks):
    row_tiles, col_tiles = ids.shape[0], ids.shape[2]
    per_bank, sketch_rows, size = bank.shape
    slots = row_tiles * col_tiles
    ids = ids.transpose(1, 2, 3, 0)
    ranks = ranks.transpose(1, 2, 3, 0)
    factors = jax.ShapeDtypeStruct((row_tiles, 1, col_tiles, 1, sketch_rows, size), F32)
    vmem = pl.BlockSpec(memory_space=pltpu.VMEM)
    smem = pl.BlockSpec(memory_space=pltpu.SMEM)
    hbm = pl.BlockSpec(memory_space=pltpu.HBM)
    dma = pltpu.SemaphoreType.DMA
    pinned = [pltpu.with_memory_space_constraint(x, pltpu.HBM) for x in (points, bank, ids, ranks)]
    y, c, residuals, whole = pl.pallas_call(
        functools.partial(kernel, rows, cols, row_tiles, col_tiles),
        out_shape=(
            factors,
            factors,
            jax.ShapeDtypeStruct((slots, 8, 128), F32),
            jax.ShapeDtypeStruct((2, 128), F32),
        ),
        in_specs=[smem, smem, hbm, hbm, hbm, hbm],
        out_specs=(vmem,) * 4,
        scratch_shapes=[
            pltpu.VMEM(points.shape, F32),
            pltpu.SMEM(ids.shape, jnp.int32),
            pltpu.SMEM(ranks.shape, jnp.int32),
            pltpu.VMEM((cols, col_tiles, 2, size), F32),
            pltpu.VMEM((cols * per_bank, sketch_rows, size), BF16),
            pltpu.VMEM((slots, size, size), BF16),
            pltpu.VMEM((slots, 8, 128), F32),
            pltpu.VMEM((2, 128), F32),
            pltpu.VMEM((rows * cols, 2, 128), F32),
            dma((5,)),
            dma((cols,)),
            dma((cols,)),
            dma((2 * cols,)),
            dma((cols,)),
            dma((rows * cols,)),
            dma((rows * cols,)),
            pltpu.SemaphoreType.REGULAR,
        ],
        compiler_params=pltpu.CompilerParams(
            collective_id=0, has_side_effects=True, vmem_limit_bytes=40 * 1024 * 1024
        ),
        name="tiles",
    )(range_length, smoothness, *pinned)
    y, c, errors, rank_total = pl.pallas_call(
        functools.partial(finish, rows, cols, row_tiles, col_tiles),
        out_shape=(
            factors,
            factors,
            jax.ShapeDtypeStruct((1, col_tiles, 1, row_tiles), F32),
            jax.ShapeDtypeStruct((1,), jnp.int32),
        ),
        in_specs=[vmem] * 4,
        out_specs=(hbm, hbm, vmem, smem),
        scratch_shapes=[dma((2, row_tiles))],
        compiler_params=pltpu.CompilerParams(vmem_limit_bytes=16 * 1024 * 1024),
        name="finish",
    )(y, c, residuals, whole)
    return y, c, errors.transpose(3, 0, 1, 2), rank_total


def solution(mesh):
    in_specs = (
        P(None, "pcol", None, None),
        P(),
        P(),
        P("pcol", None, None),
        P(None, "prow", None, "pcol"),
        P(None, "prow", None, "pcol"),
    )
    out_specs = (
        P(None, "prow", None, "pcol", None, None),
        P(None, "prow", None, "pcol", None, None),
        P(None, "prow", None, "pcol"),
        P(),
    )
    return jax.shard_map(
        functools.partial(per_device, mesh.shape["prow"], mesh.shape["pcol"]),
        mesh=mesh,
        in_specs=in_specs,
        out_specs=out_specs,
        check_vma=False,
    )
```
